32 devices in a mesh: tm: 32 (over z, y, x, core).
Axes of the slice: x: 2, y: 2, z: 4, core: 2. Of those that a mesh axis runs over, the one named last changes fastest.
Arguments:
- krylov_basis: float32 [8, 128, 32, 512], P(None, 'tm'), may hold values from -6 to 6, as said below
- vector: float32 [128, 32, 512], P('tm'), may hold values from -60 to 60
- conductance: float32 [32, 512], replicated, may hold values from 1e-05 to 0.3
Outputs:
- preconditioned: float32 [128, 32, 512], P('tm')
- next_vector: float32 [128, 32, 512], P('tm')
- coefficients: float32 [9], replicated
The draws below stay inside these ranges and needn't reach their ends.
Inputs may be any that keep to these rules, and one draw needn't show every extreme that they name: `krylov_basis`: the 8 fields are orthonormal, up to float32 rounding, under the mean over all cells of their product.
All inputs are finite; a program needn't handle non-finite values.
Results may differ from the reference program's by a relative error of at most 0.0003.
Values sent between devices are 32-bit elements.
A program may use at most 64 MiB of HBM per device.

```python
import jax
import jax.numpy as jnp
from jax import lax

SX = 32
SY = 512
LEVELS = 3
KPRIOR = 8
NT = 128


def orthonormal_fields(key):
    cell_count = NT * SX * SY
    raw_fields = jnp.clip(jax.random.normal(jax.random.fold_in(key, 11), (KPRIOR, NT, SX, SY), jnp.float32), -4.5, 4.5)
    members = []
    for position in range(KPRIOR):
        current = raw_fields[position]
        for sweep_at in range(2):
            for earlier in members:
                current = current - jnp.sum(current * earlier) / cell_count * earlier
        current = current / jnp.sqrt(jnp.sum(current * current) / cell_count)
        members.append(current)
    return jnp.stack(members)


def draw_krylov_basis(key, part):
    return orthonormal_fields(key)


def draw_vector(key, part):
    members = orthonormal_fields(key)
    magnitude = jax.random.uniform(jax.random.fold_in(key, 23), (KPRIOR,), jnp.float32, 0.5, 1.5)
    flips = jnp.where(jax.random.bernoulli(jax.random.fold_in(key, 29), 0.5, (KPRIOR,)), 1.0, -1.0)
    remainder = 0.6 * jnp.clip(jax.random.normal(jax.random.fold_in(key, 31), (NT, SX, SY), jnp.float32), -4.0, 4.0)
    mixed = jnp.einsum('k,kabc->abc', magnitude * flips, members, precision=lax.Precision.HIGHEST)
    return mixed + remainder


def draw_conductance(key, part):
    low_log = jnp.log(jnp.float32(1e-05))
    high_log = jnp.log(jnp.float32(0.3))
    return jnp.exp(jax.random.uniform(jax.random.fold_in(key, 43), (SX, SY), jnp.float32, low_log, high_log))


def setup_inputs(seed: int = 0) -> dict:
    seeds = jax.random.split(jax.random.key(seed), 4)
    return {
        "krylov_basis": draw_krylov_basis(jax.random.fold_in(seeds[3], 71), 0),
        "vector": draw_vector(jax.random.fold_in(seeds[3], 71), 0),
        "conductance": draw_conductance(jax.random.fold_in(seeds[3], 71), 0),
    }


OMEGA = 0.7
FLOOR = 0.25

def beside(volume):
    padded = jnp.pad(volume, ((0, 0), (1, 1), (1, 1)))
    return padded[:, 2:, 1:-1] + padded[:, :-2, 1:-1] + padded[:, 1:-1, 2:] + padded[:, 1:-1, :-2]

def spatial(volume, conduct):
    return volume + conduct * (4.0 * volume - beside(volume))

def time_operator(volume, conduct):
    earlier = jnp.concatenate([jnp.zeros_like(volume[:1]), volume[:-1]], axis=0)
    return spatial(volume, conduct) - earlier

def block_inverse(source, conduct):
    diagonal = 1.0 + 4.0 * conduct
    sweep_one = source / diagonal
    return (source + conduct * beside(sweep_one)) / diagonal

def coarse_march(source, conduct):
    diagonal = 1.0 + 4.0 * conduct

    def advance(carry_state, slab_in):
        carry_state = (slab_in + carry_state) / diagonal
        return (carry_state, carry_state)
    return lax.scan(advance, jnp.zeros_like(conduct), source)[1]

def vcycle(source, conduct, level_at):
    if level_at == LEVELS - 1:
        return coarse_march(source, conduct)
    smooth = OMEGA * block_inverse(source, conduct)
    remain = source - time_operator(smooth, conduct)
    coarse = remain[0::2] + remain[1::2]
    correction = vcycle(coarse, 2.0 * conduct, level_at + 1)
    smooth = smooth + jnp.repeat(correction, 2, axis=0)
    return smooth + OMEGA * block_inverse(source - time_operator(smooth, conduct), conduct)

def reference(krylov_basis, vector, conductance):
    cell_count = NT * SX * SY
    preconditioned = vcycle(vector, conductance, 0)
    applied = time_operator(preconditioned, conductance)
    weights = []
    for member in range(KPRIOR):
        weight = jnp.sum(applied * krylov_basis[member]) / cell_count
        applied = applied - weight * krylov_basis[member]
        weights.append(weight)
    length = jnp.sqrt(jnp.sum(applied * applied) / cell_count)
    next_vector = applied / jnp.maximum(length, FLOOR)
    coefficients = jnp.stack(weights + [length])
    return (preconditioned, next_vector, coefficients)
```

```python
import functools

import jax
import jax.numpy as jnp
from jax import lax
from jax.experimental import pallas as pl
from jax.experimental.pallas import tpu as pltpu
from jax.sharding import PartitionSpec as P

OMEGA = 0.7
FLOOR = 0.25
LANES = 128
MESH = pl.DeviceIdType.MESH


def to_rows(slab):
    return jnp.concatenate(
        [slab[:, at : at + LANES] for at in range(0, slab.shape[1], LANES)], axis=0
    )


def from_rows(rows, sx):
    return jnp.concatenate(
        [rows[at : at + sx] for at in range(0, rows.shape[0], sx)], axis=1
    )


def folded(x):
    parts = [
        x[a : a + 8, b : b + LANES]
        for a in range(0, x.shape[0], 8)
        for b in range(0, x.shape[1], LANES)
    ]
    while len(parts) > 1:
        parts = [parts[i] + parts[i + 1] for i in range(0, len(parts) - 1, 2)] + (
            [parts[-1]] if len(parts) % 2 else []
        )
    return parts[0]


def total(x):
    return jnp.sum(jnp.sum(folded(x), axis=0, keepdims=True), axis=1, keepdims=True)


def kernel(
    n,
    count_all,
    basis_hbm,
    vec_hbm,
    cond_hbm,
    pre_hbm,
    nxt_hbm,
    coef_ref,
    basis,
    vec,
    cond,
    pre,
    nxt,
    zout,
    zin,
    sout,
    sin,
    dchunk,
    halo_out,
    halo_in,
    late_out,
    late_in,
    part_out,
    part_in,
    load_sem,
    store_sem,
    z_sem,
    s_sem,
    h_sem,
    l_sem,
    p_sem,
):
    me = lax.axis_index("tm")
    members, m, sx, sy = basis.shape

    load_c = pltpu.make_async_copy(cond_hbm, cond, load_sem.at[0])
    load_v = pltpu.make_async_copy(vec_hbm, vec, load_sem.at[1])
    load_b = pltpu.make_async_copy(basis_hbm, basis, load_sem.at[2])
    load_c.start()
    load_v.start()
    load_b.start()

    barrier = pltpu.get_barrier_semaphore()

    def peer_of(step):
        return lax.rem(me + step, n)

    def greet(step, _):
        pl.semaphore_signal(barrier, inc=1, device_id=(peer_of(step),), device_id_type=MESH)
        return 0

    lax.fori_loop(1, n, greet, 0, unroll=n <= 32)

    def to_all(pick, into, sems):
        def send(step, _):
            peer = peer_of(step)
            pltpu.make_async_remote_copy(
                src_ref=pick(peer),
                dst_ref=into.at[me],
                send_sem=sems.at[0],
                recv_sem=sems.at[1],
                device_id=(peer,),
                device_id_type=MESH,
            ).start()
            return 0

        lax.fori_loop(1, n, send, 0, unroll=n <= 32)

    def all_of(buffer, sems):
        some = buffer.at[pl.ds(0, n - 1)]
        return pltpu.make_async_remote_copy(
            src_ref=some,
            dst_ref=some,
            send_sem=sems.at[0],
            recv_sem=sems.at[1],
            device_id=(peer_of(1),),
            device_id_type=MESH,
        )

    def to_next(src, dst, sems):
        return pltpu.make_async_remote_copy(
            src_ref=src,
            dst_ref=dst,
            send_sem=sems.at[0],
            recv_sem=sems.at[1],
            device_id=(peer_of(1),),
            device_id_type=MESH,
        )

    load_c.wait()
    c0 = cond[...]
    diag = [1.0 + 4.0 * c0, 1.0 + 8.0 * c0, 1.0 + 16.0 * c0]
    inv = [1.0 / d for d in diag]
    con = [c0, 2.0 * c0]
    row = lax.broadcasted_iota(jnp.int32, (sx, sy), 0)
    col = lax.broadcasted_iota(jnp.int32, (sx, sy), 1)

    def beside(v):
        up = jnp.where(row == 0, 0.0, pltpu.roll(v, 1, 0))
        down = jnp.where(row == sx - 1, 0.0, pltpu.roll(v, sx - 1, 0))
        left = jnp.where(col == 0, 0.0, pltpu.roll(v, 1, 1))
        right = jnp.where(col == sy - 1, 0.0, pltpu.roll(v, sy - 1, 1))
        return (up + down) + (left + right)

    def K(v, level):
        return diag[level] * v - con[level] * beside(v)

    def B(r, level):
        return (r + con[level] * beside(r * inv[level])) * (OMEGA * inv[level])

    @pl.when(me == 0)
    def _():
        halo_in[...] = jnp.zeros_like(halo_in)
        late_in[...] = jnp.zeros_like(late_in)

    load_v.wait()
    r = [vec[i] for i in range(m)]
    u = [B(r[i], 0) for i in range(m)]
    s = [r[0] - K(u[0], 0)] + [r[i] - K(u[i], 0) + u[i - 1] for i in range(1, m)]
    cl = [s[0] + s[1], s[2] + s[3]]
    v0 = B(cl[0], 1)
    v1 = B(cl[1], 1)
    t0 = cl[0] - K(v0, 1)
    t1 = cl[1] - K(v1, 1) + v0
    q_next = B(u[3], 1)
    x_next = u[3] - K(q_next, 1) + q_next + v1
    dl = (t0 + t1) * inv[2]
    zout[...] = to_rows(dl + x_next).reshape(zout.shape)
    dchunk[...] = to_rows(inv[2]).reshape(dchunk.shape)
    halo_out[0] = u[3]
    halo_out[1] = v1

    pl.semaphore_wait(barrier, n - 1)
    to_all(lambda peer: zout.at[peer], zin, z_sem)

    halo = to_next(halo_out, halo_in, h_sem)

    @pl.when(me < n - 1)
    def _():
        halo.start()

    zin[me] = zout[me]
    dmine = dchunk[me]
    all_of(zin, z_sem).wait_recv()

    def advance(k, state):
        sout[k] = state
        return (zin[k] + state) * dmine

    lax.fori_loop(0, n, advance, jnp.zeros_like(dmine), unroll=n <= 32)
    to_all(lambda peer: sout.at[peer], sin, s_sem)
    sin[me] = sout[me]

    @pl.when(me > 0)
    def _():
        halo.wait_recv()

    p = halo_in[0]
    q = B(p, 1)
    a = p - K(q, 1) + halo_in[1]
    x_mine = a + q
    e1 = v1 + B(t1 + q, 1)
    n2 = u[2] + e1
    n3 = u[3] + e1
    res3 = n3 + B(r[3] - K(n3, 0) + n2, 0)
    late_out[0] = n3
    late_out[1] = res3
    late = to_next(late_out, late_in, l_sem)

    @pl.when(me < n - 1)
    def _():
        late.start()

    e0 = v0 + q + B(t0 + a, 1)
    n0 = u[0] + e0
    n1 = u[1] + e0
    res1 = n1 + B(r[1] - K(n1, 0) + n0, 0)
    res2 = n2 + B(r[2] - K(n2, 0) + n1, 0)
    m0 = r[0] - K(n0, 0)

    load_b.wait()
    lane = lax.broadcasted_iota(jnp.int32, (1, LANES), 1)
    part = jnp.zeros((1, LANES), jnp.float32)
    for j in range(members):
        square = basis[j, 0] * basis[j, 0]
        for i in range(1, m):
            square += basis[j, i] * basis[j, i]
        part = jnp.where(lane == members + 1 + j, total(square), part)

    @pl.when(me > 0)
    def _():
        late.wait_recv()

    res0 = n0 + B(m0 + late_in[0], 0)
    resp = late_in[1]

    all_of(sin, s_sem).wait_recv()
    entering = from_rows(sin[...].reshape(sx * sy // LANES, LANES), sx)
    e = dl + entering
    ep = diag[2] * entering - x_mine
    ke = K(e, 1)
    f0 = e - B(ke - ep, 1)
    f1 = e - B(ke - e, 1)
    fp = ep - B(K(ep, 1) - ep, 1)
    k0 = K(f0, 0)
    k1 = K(f1, 0)
    res0 += f0 - B(k0 - fp, 0)
    res1 += f0 - B(k0 - f0, 0)
    res2 += f1 - B(k1 - f0, 0)
    res3 += f1 - B(k1 - f1, 0)
    resp += fp - B(K(fp, 0) - fp, 0)
    res = [res0, res1, res2, res3]
    for i in range(m):
        pre[i] = res[i]
    store_p = pltpu.make_async_copy(pre, pre_hbm, store_sem.at[0])
    store_p.start()

    w = [K(res[i], 0) - (res[i - 1] if i else resp) for i in range(m)]
    for j in range(members):
        dot = w[0] * basis[j, 0]
        for i in range(1, m):
            dot += w[i] * basis[j, i]
        part = jnp.where(lane == j, total(dot), part)
    square = w[0] * w[0]
    for i in range(1, m):
        square += w[i] * w[i]
    part = jnp.where(lane == members, total(square), part)
    part_out[...] = part
    to_all(lambda peer: part_out, part_in, p_sem)
    part_in[me] = part
    all_of(part_in, p_sem).wait_recv()
    sums = jnp.sum(part_in[...], axis=0) * (1.0 / count_all)

    weights = [sums[:, j : j + 1] for j in range(members)]
    left = sums[:, members : members + 1]
    for j in range(members):
        gram = sums[:, members + 1 + j : members + 2 + j]
        left -= weights[j] * weights[j] * (2.0 - gram)
    length = jnp.sqrt(jnp.maximum(left, 0.0))
    scale = 1.0 / jnp.maximum(length, FLOOR)
    for i in range(m):
        out = w[i]
        for j in range(members):
            out -= weights[j] * basis[j, i]
        nxt[i] = out * scale
    store_n = pltpu.make_async_copy(nxt, nxt_hbm, store_sem.at[1])
    store_n.start()
    for j in range(members):
        coef_ref[j] = weights[j][0, 0]
    coef_ref[members] = length[0, 0]

    all_of(zin, z_sem).wait_send()
    all_of(sin, s_sem).wait_send()
    all_of(part_in, p_sem).wait_send()

    @pl.when(me < n - 1)
    def _():
        halo.wait_send()
        late.wait_send()

    store_p.wait()
    store_n.wait()


def solution(mesh):
    n = mesh.shape["tm"]

    def on_device(krylov_basis, vector, conductance):
        members, m, sx, sy = krylov_basis.shape
        assert m == 4
        rows = sx * sy // LANES // n
        chunk = pltpu.VMEM((n, rows, LANES), jnp.float32)
        slabs = lambda k: pltpu.VMEM((k, sx, sy), jnp.float32)
        pair = pltpu.SemaphoreType.DMA((2,))
        anywhere = pl.BlockSpec(memory_space=pl.ANY)
        return pl.pallas_call(
            functools.partial(kernel, n, m * n * sx * sy),
            out_shape=(
                jax.ShapeDtypeStruct(vector.shape, jnp.float32),
                jax.ShapeDtypeStruct(vector.shape, jnp.float32),
                jax.ShapeDtypeStruct((members + 1,), jnp.float32),
            ),
            in_specs=[anywhere] * 3,
            out_specs=(anywhere, anywhere, pl.BlockSpec(memory_space=pltpu.SMEM)),
            scratch_shapes=[
                pltpu.VMEM(krylov_basis.shape, jnp.float32),
                slabs(m),
                pltpu.VMEM((sx, sy), jnp.float32),
                slabs(m),
                slabs(m),
                chunk,
                chunk,
                chunk,
                chunk,
                chunk,
                slabs(2),
                slabs(2),
                slabs(2),
                slabs(2),
                pltpu.VMEM((1, LANES), jnp.float32),
                pltpu.VMEM((n, 1, LANES), jnp.float32),
                pltpu.SemaphoreType.DMA((3,)),
                pair,
                pair,
                pair,
                pair,
                pair,
                pair,
            ],
            compiler_params=pltpu.CompilerParams(collective_id=0, has_side_effects=True),
            name="arnoldi_step",
        )(krylov_basis, vector, conductance)

    return jax.shard_map(
        on_device,
        mesh=mesh,
        in_specs=(P(None, "tm", None, None), P("tm", None, None), P()),
        out_specs=(P("tm", None, None), P("tm", None, None), P()),
        check_vma=False,
    )
```

```python
import functools

import jax
import jax.numpy as jnp
from jax import lax
from jax.experimental import pallas as pl
from jax.experimental.pallas import tpu as pltpu
from jax.sharding import PartitionSpec as P

OMEGA = 0.7
FLOOR = 0.25
LANES = 128
MESH = pl.DeviceIdType.MESH


def to_rows(slab):
    return jnp.concatenate(
        [slab[:, at : at + LANES] for at in range(0, slab.shape[1], LANES)], axis=0
    )


def from_rows(rows, sx):
    return jnp.concatenate(
        [rows[at : at + sx] for at in range(0, rows.shape[0], sx)], axis=1
    )


def folded(x):
    parts = [
        x[a : a + 8, b : b + LANES]
        for a in range(0, x.shape[0], 8)
        for b in range(0, x.shape[1], LANES)
    ]
    while len(parts) > 1:
        parts = [parts[i] + parts[i + 1] for i in range(0, len(parts) - 1, 2)] + (
            [parts[-1]] if len(parts) % 2 else []
        )
    return parts[0]


def total(x):
    return jnp.sum(jnp.sum(folded(x), axis=0, keepdims=True), axis=1, keepdims=True)


def kernel(
    n,
    count_all,
    basis_hbm,
    vec_hbm,
    cond_hbm,
    pre,
    w_ref,
    sums_ref,
    basis,
    vec,
    cond,
    zout,
    zin,
    sout,
    sin,
    dchunk,
    halo_out,
    halo_in,
    late_out,
    late_in,
    part_out,
    part_in,
    load_sem,
    z_sem,
    s_sem,
    h_sem,
    l_sem,
    p_sem,
):
    me = lax.axis_index("tm")
    members, m, sx, sy = basis.shape

    load_c = pltpu.make_async_copy(cond_hbm, cond, load_sem.at[0])
    load_v = pltpu.make_async_copy(vec_hbm, vec, load_sem.at[1])
    load_b = pltpu.make_async_copy(basis_hbm, basis, load_sem.at[2])
    load_c.start()
    load_v.start()
    load_b.start()

    barrier = pltpu.get_barrier_semaphore()

    def peer_of(step):
        return lax.rem(me + step, n)

    def greet(step, _):
        pl.semaphore_signal(barrier, inc=1, device_id=(peer_of(step),), device_id_type=MESH)
        return 0

    lax.fori_loop(1, n, greet, 0, unroll=n <= 32)

    def to_all(pick, into, sems):
        def send(step, _):
            peer = peer_of(step)
            pltpu.make_async_remote_copy(
                src_ref=pick(peer),
                dst_ref=into.at[me],
                send_sem=sems.at[0],
                recv_sem=sems.at[1],
                device_id=(peer,),
                device_id_type=MESH,
            ).start()
            return 0

        lax.fori_loop(1, n, send, 0, unroll=n <= 32)

    def all_of(buffer, sems):
        some = buffer.at[pl.ds(0, n - 1)]
        return pltpu.make_async_remote_copy(
            src_ref=some,
            dst_ref=some,
            send_sem=sems.at[0],
            recv_sem=sems.at[1],
            device_id=(peer_of(1),),
            device_id_type=MESH,
        )

    def to_next(src, dst, sems):
        return pltpu.make_async_remote_copy(
            src_ref=src,
            dst_ref=dst,
            send_sem=sems.at[0],
            recv_sem=sems.at[1],
            device_id=(peer_of(1),),
            device_id_type=MESH,
        )

    load_c.wait()
    c0 = cond[...]
    diag = [1.0 + 4.0 * c0, 1.0 + 8.0 * c0, 1.0 + 16.0 * c0]
    inv = [1.0 / d for d in diag]
    con = [c0, 2.0 * c0]
    row = lax.broadcasted_iota(jnp.int32, (sx, sy), 0)
    col = lax.broadcasted_iota(jnp.int32, (sx, sy), 1)

    def beside(v):
        up = jnp.where(row == 0, 0.0, pltpu.roll(v, 1, 0))
        down = jnp.where(row == sx - 1, 0.0, pltpu.roll(v, sx - 1, 0))
        left = jnp.where(col == 0, 0.0, pltpu.roll(v, 1, 1))
        right = jnp.where(col == sy - 1, 0.0, pltpu.roll(v, sy - 1, 1))
        return (up + down) + (left + right)

    def K(v, level):
        return diag[level] * v - con[level] * beside(v)

    def B(r, level):
        return (r + con[level] * beside(r * inv[level])) * (OMEGA * inv[level])

    @pl.when(me == 0)
    def _():
        halo_in[...] = jnp.zeros_like(halo_in)
        late_in[...] = jnp.zeros_like(late_in)

    load_v.wait()
    r = [vec[i] for i in range(m)]
    u = [B(r[i], 0) for i in range(m)]
    s = [r[0] - K(u[0], 0)] + [r[i] - K(u[i], 0) + u[i - 1] for i in range(1, m)]
    cl = [s[0] + s[1], s[2] + s[3]]
    v0 = B(cl[0], 1)
    v1 = B(cl[1], 1)
    t0 = cl[0] - K(v0, 1)
    t1 = cl[1] - K(v1, 1) + v0
    q_next = B(u[3], 1)
    x_next = u[3] - K(q_next, 1) + q_next + v1
    dl = (t0 + t1) * inv[2]
    zout[...] = to_rows(dl + x_next).reshape(zout.shape)
    dchunk[...] = to_rows(inv[2]).reshape(dchunk.shape)
    halo_out[0] = u[3]
    halo_out[1] = v1

    pl.semaphore_wait(barrier, n - 1)
    to_all(lambda peer: zout.at[peer], zin, z_sem)

    halo = to_next(halo_out, halo_in, h_sem)

    @pl.when(me < n - 1)
    def _():
        halo.start()

    zin[me] = zout[me]
    dmine = dchunk[me]
    all_of(zin, z_sem).wait_recv()

    def advance(k, state):
        sout[k] = state
        return (zin[k] + state) * dmine

    lax.fori_loop(0, n, advance, jnp.zeros_like(dmine), unroll=n <= 32)
    to_all(lambda peer: sout.at[peer], sin, s_sem)
    sin[me] = sout[me]

    @pl.when(me > 0)
    def _():
        halo.wait_recv()

    p = halo_in[0]
    q = B(p, 1)
    a = p - K(q, 1) + halo_in[1]
    x_mine = a + q
    e1 = v1 + B(t1 + q, 1)
    n2 = u[2] + e1
    n3 = u[3] + e1
    res3 = n3 + B(r[3] - K(n3, 0) + n2, 0)
    late_out[0] = n3
    late_out[1] = res3
    late = to_next(late_out, late_in, l_sem)

    @pl.when(me < n - 1)
    def _():
        late.start()

    e0 = v0 + q + B(t0 + a, 1)
    n0 = u[0] + e0
    n1 = u[1] + e0
    res1 = n1 + B(r[1] - K(n1, 0) + n0, 0)
    res2 = n2 + B(r[2] - K(n2, 0) + n1, 0)
    m0 = r[0] - K(n0, 0)

    load_b.wait()
    lane = lax.broadcasted_iota(jnp.int32, (1, LANES), 1)
    part = jnp.zeros((1, LANES), jnp.float32)
    for j in range(members):
        square = basis[j, 0] * basis[j, 0]
        for i in range(1, m):
            square += basis[j, i] * basis[j, i]
        part = jnp.where(lane == members + 1 + j, total(square), part)

    @pl.when(me > 0)
    def _():
        late.wait_recv()

    res0 = n0 + B(m0 + late_in[0], 0)
    resp = late_in[1]

    all_of(sin, s_sem).wait_recv()
    entering = from_rows(sin[...].reshape(sx * sy // LANES, LANES), sx)
    e = dl + entering
    ep = diag[2] * entering - x_mine
    ke = K(e, 1)
    f0 = e - B(ke - ep, 1)
    f1 = e - B(ke - e, 1)
    fp = ep - B(K(ep, 1) - ep, 1)
    k0 = K(f0, 0)
    k1 = K(f1, 0)
    res0 += f0 - B(k0 - fp, 0)
    res1 += f0 - B(k0 - f0, 0)
    res2 += f1 - B(k1 - f0, 0)
    res3 += f1 - B(k1 - f1, 0)
    resp += fp - B(K(fp, 0) - fp, 0)
    res = [res0, res1, res2, res3]
    for i in range(m):
        pre[i] = res[i]

    w = [K(res[i], 0) - (res[i - 1] if i else resp) for i in range(m)]
    for i in range(m):
        w_ref[i] = w[i]
    for j in range(members):
        dot = w[0] * basis[j, 0]
        for i in range(1, m):
            dot += w[i] * basis[j, i]
        part = jnp.where(lane == j, total(dot), part)
    square = w[0] * w[0]
    for i in range(1, m):
        square += w[i] * w[i]
    part = jnp.where(lane == members, total(square), part)
    part_out[...] = part
    to_all(lambda peer: part_out, part_in, p_sem)
    part_in[me] = part
    all_of(part_in, p_sem).wait_recv()
    sums_ref[...] = jnp.sum(part_in[...], axis=0) * (1.0 / count_all)

    all_of(zin, z_sem).wait_send()
    all_of(sin, s_sem).wait_send()
    all_of(part_in, p_sem).wait_send()

    @pl.when(me < n - 1)
    def _():
        halo.wait_send()
        late.wait_send()


def finish(pre, w, sums_ref, basis, pre_hbm, nxt_hbm, coef_ref, nxt, store_sem):
    members, m = basis.shape[:2]
    store_p = pltpu.make_async_copy(pre, pre_hbm, store_sem.at[0])
    store_p.start()
    sums = sums_ref[...]
    weights = [sums[:, j : j + 1] for j in range(members)]
    left = sums[:, members : members + 1]
    for j in range(members):
        gram = sums[:, members + 1 + j : members + 2 + j]
        left -= weights[j] * weights[j] * (2.0 - gram)
    length = jnp.sqrt(jnp.maximum(left, 0.0))
    scale = 1.0 / jnp.maximum(length, FLOOR)
    stores = []
    for i in range(m):
        out = w[i]
        for j in range(members):
            out -= weights[j] * basis[j, i]
        nxt[i] = out * scale
        stores.append(pltpu.make_async_copy(nxt.at[i], nxt_hbm.at[i], store_sem.at[i + 1]))
        stores[-1].start()
    for j in range(members):
        coef_ref[j] = weights[j][0, 0]
    coef_ref[members] = length[0, 0]
    store_p.wait()
    for store in stores:
        store.wait()


def solution(mesh):
    n = mesh.shape["tm"]

    def on_device(krylov_basis, vector, conductance):
        members, m, sx, sy = krylov_basis.shape
        assert m == 4
        rows = sx * sy // LANES // n
        chunk = pltpu.VMEM((n, rows, LANES), jnp.float32)
        slabs = lambda k: pltpu.VMEM((k, sx, sy), jnp.float32)
        pair = pltpu.SemaphoreType.DMA((2,))
        anywhere = pl.BlockSpec(memory_space=pl.ANY)
        inside = pl.BlockSpec(memory_space=pltpu.VMEM)
        pre, w, sums, basis = pl.pallas_call(
            functools.partial(kernel, n, m * n * sx * sy),
            out_shape=(
                pltpu.VMEM(vector.shape, jnp.float32),
                pltpu.VMEM(vector.shape, jnp.float32),
                pltpu.VMEM((1, LANES), jnp.float32),
                pltpu.VMEM(krylov_basis.shape, jnp.float32),
            ),
            in_specs=[anywhere] * 3,
            out_specs=(inside,) * 4,
            scratch_shapes=[
                slabs(m),
                pltpu.VMEM((sx, sy), jnp.float32),
                chunk,
                chunk,
                chunk,
                chunk,
                chunk,
                slabs(2),
                slabs(2),
                slabs(2),
                slabs(2),
                pltpu.VMEM((1, LANES), jnp.float32),
                pltpu.VMEM((n, 1, LANES), jnp.float32),
                pltpu.SemaphoreType.DMA((3,)),
                pair,
                pair,
                pair,
                pair,
                pair,
            ],
            compiler_params=pltpu.CompilerParams(collective_id=0, has_side_effects=True),
            name="arnoldi_step",
        )(krylov_basis, vector, conductance)
        held = [pltpu.with_memory_space_constraint(x, pltpu.VMEM) for x in (pre, w, sums, basis)]
        return pl.pallas_call(
            finish,
            out_shape=(
                jax.ShapeDtypeStruct(vector.shape, jnp.float32),
                jax.ShapeDtypeStruct(vector.shape, jnp.float32),
                jax.ShapeDtypeStruct((members + 1,), jnp.float32),
            ),
            in_specs=[inside] * 4,
            out_specs=(anywhere, anywhere, pl.BlockSpec(memory_space=pltpu.SMEM)),
            scratch_shapes=[slabs(m), pltpu.SemaphoreType.DMA((m + 1,))],
            name="next_vector",
        )(*held)

    return jax.shard_map(
        on_device,
        mesh=mesh,
        in_specs=(P(None, "tm", None, None), P("tm", None, None), P()),
        out_specs=(P("tm", None, None), P("tm", None, None), P()),
        check_vma=False,
    )
```

```python
import functools

import jax
import jax.numpy as jnp
from jax import lax
from jax.experimental import pallas as pl
from jax.experimental.pallas import tpu as pltpu
from jax.sharding import PartitionSpec as P

OMEGA = 0.7
FLOOR = 0.25
LANES = 128
MESH = pl.DeviceIdType.MESH


def to_rows(slab):
    return jnp.concatenate(
        [slab[:, at : at + LANES] for at in range(0, slab.shape[1], LANES)], axis=0
    )


def from_rows(rows, sx):
    return jnp.concatenate(
        [rows[at : at + sx] for at in range(0, rows.shape[0], sx)], axis=1
    )


def folded(x):
    parts = [
        x[a : a + 8, b : b + LANES]
        for a in range(0, x.shape[0], 8)
        for b in range(0, x.shape[1], LANES)
    ]
    while len(parts) > 1:
        parts = [parts[i] + parts[i + 1] for i in range(0, len(parts) - 1, 2)] + (
            [parts[-1]] if len(parts) % 2 else []
        )
    return parts[0]


def total(x):
    return jnp.sum(jnp.sum(folded(x), axis=0, keepdims=True), axis=1, keepdims=True)


def kernel(
    n,
    count_all,
    basis_hbm,
    vec_hbm,
    cond_hbm,
    pre,
    w_ref,
    sums_ref,
    basis,
    vec,
    cond,
    zout,
    zin,
    sout,
    sin,
    dchunk,
    halo_out,
    halo_in,
    late_out,
    late_in,
    part_out,
    part_in,
    load_sem,
    z_sem,
    s_sem,
    h_sem,
    l_sem,
    p_sem,
):
    me = lax.axis_index("tm")
    members, m, sx, sy = basis.shape

    load_c = pltpu.make_async_copy(cond_hbm, cond, load_sem.at[0])
    load_v = pltpu.make_async_copy(vec_hbm, vec, load_sem.at[1])
    load_b = pltpu.make_async_copy(basis_hbm, basis, load_sem.at[2])
    load_c.start()
    load_v.start()
    load_b.start()

    barrier = pltpu.get_barrier_semaphore()

    def peer_of(step):
        return lax.rem(me + step, n)

    def greet(step, _):
        pl.semaphore_signal(barrier, inc=1, device_id=(peer_of(step),), device_id_type=MESH)
        return 0

    lax.fori_loop(1, n, greet, 0, unroll=n <= 32)

    def to_all(pick, into, sems):
        def send(step, _):
            peer = peer_of(step)
            pltpu.make_async_remote_copy(
                src_ref=pick(peer),
                dst_ref=into,
                send_sem=sems.at[0],
                recv_sem=sems.at[1],
                device_id=(peer,),
                device_id_type=MESH,
            ).start()
            return 0

        lax.fori_loop(1, n, send, 0, unroll=n <= 32)

    def all_of(buffer, count, sems):
        some = buffer.at[pl.ds(0, count)]
        return pltpu.make_async_remote_copy(
            src_ref=some,
            dst_ref=some,
            send_sem=sems.at[0],
            recv_sem=sems.at[1],
            device_id=(peer_of(1),),
            device_id_type=MESH,
        )

    def to_next(src, dst, sems):
        return pltpu.make_async_remote_copy(
            src_ref=src,
            dst_ref=dst,
            send_sem=sems.at[0],
            recv_sem=sems.at[1],
            device_id=(peer_of(1),),
            device_id_type=MESH,
        )

    load_c.wait()
    c0 = cond[...]
    diag = [1.0 + 4.0 * c0, 1.0 + 8.0 * c0, 1.0 + 16.0 * c0]
    inv = [1.0 / d for d in diag]
    con = [c0, 2.0 * c0]
    row = lax.broadcasted_iota(jnp.int32, (sx, sy), 0)
    col = lax.broadcasted_iota(jnp.int32, (sx, sy), 1)

    def beside(v):
        up = jnp.where(row == 0, 0.0, pltpu.roll(v, 1, 0))
        down = jnp.where(row == sx - 1, 0.0, pltpu.roll(v, sx - 1, 0))
        left = jnp.where(col == 0, 0.0, pltpu.roll(v, 1, 1))
        right = jnp.where(col == sy - 1, 0.0, pltpu.roll(v, sy - 1, 1))
        return (up + down) + (left + right)

    def K(v, level):
        return diag[level] * v - con[level] * beside(v)

    def B(r, level):
        return (r + con[level] * beside(r * inv[level])) * (OMEGA * inv[level])

    @pl.when(me == 0)
    def _():
        halo_in[...] = jnp.zeros_like(halo_in)
        late_in[...] = jnp.zeros_like(late_in)

    load_v.wait()
    r = [vec[i] for i in range(m)]
    u = [B(r[i], 0) for i in range(m)]
    s = [r[0] - K(u[0], 0)] + [r[i] - K(u[i], 0) + u[i - 1] for i in range(1, m)]
    cl = [s[0] + s[1], s[2] + s[3]]
    v0 = B(cl[0], 1)
    v1 = B(cl[1], 1)
    t0 = cl[0] - K(v0, 1)
    t1 = cl[1] - K(v1, 1) + v0
    q_next = B(u[3], 1)
    x_next = u[3] - K(q_next, 1) + q_next + v1
    dl = (t0 + t1) * inv[2]
    zout[...] = to_rows(dl + x_next).reshape(zout.shape)
    dchunk[...] = to_rows(inv[2]).reshape(dchunk.shape)
    halo_out[0] = u[3]
    halo_out[1] = v1

    owners = n // 2
    first = n // 4
    mine = lax.rem(me - first + n, owners)
    owner = jnp.logical_and(me >= first, me < first + owners)

    pl.semaphore_wait(barrier, n - 1)

    def to_owner(step, _):
        chunk = lax.rem(mine + step, owners)
        pltpu.make_async_remote_copy(
            src_ref=zout.at[chunk],
            dst_ref=zin.at[me],
            send_sem=z_sem.at[0],
            recv_sem=z_sem.at[1],
            device_id=(first + chunk,),
            device_id_type=MESH,
        ).start()
        return 0

    @pl.when(jnp.logical_not(owner))
    def _():
        to_owner(0, 0)

    lax.fori_loop(1, owners, to_owner, 0, unroll=n <= 32)

    halo = to_next(halo_out, halo_in, h_sem)

    @pl.when(me < n - 1)
    def _():
        halo.start()

    @pl.when(owner)
    def _():
        zin[me] = zout[mine]
        dmine = dchunk[mine]
        all_of(zin, n - 1, z_sem).wait_recv()

        def advance(k, state):
            sout[k] = state
            return (zin[k] + state) * dmine

        lax.fori_loop(0, n, advance, jnp.zeros_like(dmine), unroll=n <= 32)
        to_all(lambda peer: sout.at[peer], sin.at[mine], s_sem)
        sin[mine] = sout[me]

    @pl.when(me > 0)
    def _():
        halo.wait_recv()

    p = halo_in[0]
    q = B(p, 1)
    a = p - K(q, 1) + halo_in[1]
    x_mine = a + q
    e1 = v1 + B(t1 + q, 1)
    n2 = u[2] + e1
    n3 = u[3] + e1
    res3 = n3 + B(r[3] - K(n3, 0) + n2, 0)
    late_out[0] = n3
    late_out[1] = res3
    late = to_next(late_out, late_in, l_sem)

    @pl.when(me < n - 1)
    def _():
        late.start()

    e0 = v0 + q + B(t0 + a, 1)
    n0 = u[0] + e0
    n1 = u[1] + e0
    res1 = n1 + B(r[1] - K(n1, 0) + n0, 0)
    res2 = n2 + B(r[2] - K(n2, 0) + n1, 0)
    m0 = r[0] - K(n0, 0)

    load_b.wait()
    lane = lax.broadcasted_iota(jnp.int32, (1, LANES), 1)
    part = jnp.zeros((1, LANES), jnp.float32)
    for j in range(members):
        square = basis[j, 0] * basis[j, 0]
        for i in range(1, m):
            square += basis[j, i] * basis[j, i]
        part = jnp.where(lane == members + 1 + j, total(square), part)

    @pl.when(me > 0)
    def _():
        late.wait_recv()

    res0 = n0 + B(m0 + late_in[0], 0)
    resp = late_in[1]

    @pl.when(owner)
    def _():
        all_of(sin, owners - 1, s_sem).wait_recv()

    @pl.when(jnp.logical_not(owner))
    def _():
        all_of(sin, owners, s_sem).wait_recv()

    entering = from_rows(sin[...].reshape(sx * sy // LANES, LANES), sx)
    e = dl + entering
    ep = diag[2] * entering - x_mine
    ke = K(e, 1)
    f0 = e - B(ke - ep, 1)
    f1 = e - B(ke - e, 1)
    fp = ep - B(K(ep, 1) - ep, 1)
    k0 = K(f0, 0)
    k1 = K(f1, 0)
    res0 += f0 - B(k0 - fp, 0)
    res1 += f0 - B(k0 - f0, 0)
    res2 += f1 - B(k1 - f0, 0)
    res3 += f1 - B(k1 - f1, 0)
    resp += fp - B(K(fp, 0) - fp, 0)
    res = [res0, res1, res2, res3]
    for i in range(m):
        pre[i] = res[i]

    w = [K(res[i], 0) - (res[i - 1] if i else resp) for i in range(m)]
    for i in range(m):
        w_ref[i] = w[i]
    for j in range(members):
        dot = w[0] * basis[j, 0]
        for i in range(1, m):
            dot += w[i] * basis[j, i]
        part = jnp.where(lane == j, total(dot), part)
    square = w[0] * w[0]
    for i in range(1, m):
        square += w[i] * w[i]
    part = jnp.where(lane == members, total(square), part)
    part_out[...] = part
    to_all(lambda peer: part_out, part_in.at[me], p_sem)
    part_in[me] = part
    all_of(part_in, n - 1, p_sem).wait_recv()
    sums_ref[...] = jnp.sum(part_in[...], axis=0) * (1.0 / count_all)

    @pl.when(owner)
    def _():
        all_of(zout, owners - 1, z_sem).wait_send()
        all_of(sout, n - 1, s_sem).wait_send()

    @pl.when(jnp.logical_not(owner))
    def _():
        all_of(zout, owners, z_sem).wait_send()

    all_of(part_in, n - 1, p_sem).wait_send()

    @pl.when(me < n - 1)
    def _():
        halo.wait_send()
        late.wait_send()


def finish(pre, w, sums_ref, basis, pre_hbm, nxt_hbm, coef_ref, nxt, store_sem):
    members, m = basis.shape[:2]
    store_p = pltpu.make_async_copy(pre, pre_hbm, store_sem.at[0])
    store_p.start()
    sums = sums_ref[...]
    weights = [sums[:, j : j + 1] for j in range(members)]
    left = sums[:, members : members + 1]
    for j in range(members):
        gram = sums[:, members + 1 + j : members + 2 + j]
        left -= weights[j] * weights[j] * (2.0 - gram)
    length = jnp.sqrt(jnp.maximum(left, 0.0))
    scale = 1.0 / jnp.maximum(length, FLOOR)
    stores = []
    for i in range(m):
        out = w[i]
        for j in range(members):
            out -= weights[j] * basis[j, i]
        nxt[i] = out * scale
        stores.append(pltpu.make_async_copy(nxt.at[i], nxt_hbm.at[i], store_sem.at[i + 1]))
        stores[-1].start()
    for j in range(members):
        coef_ref[j] = weights[j][0, 0]
    coef_ref[members] = length[0, 0]
    store_p.wait()
    for store in stores:
        store.wait()


def solution(mesh):
    n = mesh.shape["tm"]

    def on_device(krylov_basis, vector, conductance):
        members, m, sx, sy = krylov_basis.shape
        assert m == 4
        owners = n // 2
        rows = sx * sy // LANES // owners
        chunk = pltpu.VMEM((owners, rows, LANES), jnp.float32)
        steps = pltpu.VMEM((n, rows, LANES), jnp.float32)
        slabs = lambda k: pltpu.VMEM((k, sx, sy), jnp.float32)
        pair = pltpu.SemaphoreType.DMA((2,))
        anywhere = pl.BlockSpec(memory_space=pl.ANY)
        inside = pl.BlockSpec(memory_space=pltpu.VMEM)
        pre, w, sums, basis = pl.pallas_call(
            functools.partial(kernel, n, m * n * sx * sy),
            out_shape=(
                pltpu.VMEM(vector.shape, jnp.float32),
                pltpu.VMEM(vector.shape, jnp.float32),
                pltpu.VMEM((1, LANES), jnp.float32),
                pltpu.VMEM(krylov_basis.shape, jnp.float32),
            ),
            in_specs=[anywhere] * 3,
            out_specs=(inside,) * 4,
            scratch_shapes=[
                slabs(m),
                pltpu.VMEM((sx, sy), jnp.float32),
                chunk,
                steps,
                steps,
                chunk,
                chunk,
                slabs(2),
                slabs(2),
                slabs(2),
                slabs(2),
                pltpu.VMEM((1, LANES), jnp.float32),
                pltpu.VMEM((n, 1, LANES), jnp.float32),
                pltpu.SemaphoreType.DMA((3,)),
                pair,
                pair,
                pair,
                pair,
                pair,
            ],
            compiler_params=pltpu.CompilerParams(collective_id=0, has_side_effects=True),
            name="arnoldi_step",
        )(krylov_basis, vector, conductance)
        held = [pltpu.with_memory_space_constraint(x, pltpu.VMEM) for x in (pre, w, sums, basis)]
        return pl.pallas_call(
            finish,
            out_shape=(
                jax.ShapeDtypeStruct(vector.shape, jnp.float32),
                jax.ShapeDtypeStruct(vector.shape, jnp.float32),
                jax.ShapeDtypeStruct((members + 1,), jnp.float32),
            ),
            in_specs=[inside] * 4,
            out_specs=(anywhere, anywhere, pl.BlockSpec(memory_space=pltpu.SMEM)),
            scratch_shapes=[slabs(m), pltpu.SemaphoreType.DMA((m + 1,))],
            name="next_vector",
        )(*held)

    return jax.shard_map(
        on_device,
        mesh=mesh,
        in_specs=(P(None, "tm", None, None), P("tm", None, None), P()),
        out_specs=(P("tm", None, None), P("tm", None, None), P()),
        check_vma=False,
    )
```
